32 devices in a mesh: crop: 8 (over z, core), branch: 2 (over y), dap: 2 (over x).
Axes of the slice: x: 2, y: 2, z: 4, core: 2. Of those that a mesh axis runs over, the one named last changes fastest.
Arguments:
- homolog_matrix: bfloat16 [256, 64, 256], P(('crop', 'dap')), parts along dimension 0, may hold values from -6 to 6
- homolog_entry_flags: int32 [256, 64], P(('crop', 'dap')), parts along dimension 0, may hold values 0 or 1
- couple_matrix: bfloat16 [512, 64, 128], P(('crop', 'dap')), parts along dimension 0, may hold values from -6 to 6
- window_amino_flags: int32 [512], P('crop'), parts along dimension 0, may hold values from 0 to 1, as said below
- pairwise_standardize_scaling: float32 [256], replicated, may hold values from 0.1 to 1.9
- pairwise_standardize_offset: float32 [256], replicated, may hold values from -3 to 3
- pairwise_factor_matrices: bfloat16 [256, 64], replicated, may hold values from -0.375 to 0.375
- pairwise_final_matrix: bfloat16 [1024, 128], replicated, may hold values from -0.75 to 0.75
- pairwise_final_offset: float32 [128], replicated, may hold values from -3 to 3
- trimul_entry_standardize_scaling: float32 [128], replicated, may hold values from 0.1 to 1.9
- trimul_entry_standardize_offset: float32 [128], replicated, may hold values from -3 to 3
- trimul_entry_matrices: bfloat16 [128, 640], replicated, may hold values from -0.5 to 0.5
- trimul_entry_offsets: float32 [640], replicated, may hold values from -3 to 3
- trimul_final_standardize_scaling: float32 [128], replicated, may hold values from 0.1 to 1.9
- trimul_final_standardize_offset: float32 [128], replicated, may hold values from -3 to 3
- trimul_final_matrix: bfloat16 [128, 128], replicated, may hold values from -0.5 to 0.5
- trimul_final_offset: float32 [128], replicated, may hold values from -3 to 3
Outputs:
- pair_out: bfloat16 [512, 64, 128], P(('crop', 'dap'), 'branch'), parts along dimension 0
The draws below stay inside these ranges and needn't reach their ends.
There are 8 independent parts, one for each index of `crop`. The reference program is written for one: setup_inputs(seed, part) draws one part's arguments, and reference() takes and returns one part's arrays. A program takes and returns all parts, laid end to end along the dimension named above; an argument that names none is the same for every part. Nothing has to cross between parts.
Inputs may be any that keep to these rules, and one draw needn't show every extreme that they name: `window_amino_flags`: 1 on the first residues of the crop and 0 on the rest, with at least 32 ones.
All inputs are finite; a program needn't handle non-finite values. No bound on the sum of `homolog_entry_flags` on one device may be relied on, other than what follows from the above.
Results may differ from the reference program's by a relative error of at most 0.0057.
Values may be sent and summed in bfloat16 or wider, within the bound.
A program may use at most 64 MiB of HBM per device.

```python
import jax
import jax.numpy as jnp
from jax import lax

HOMOLOG_FEATURES = 256
CZ = 128
PAIRWISE_FEATURES = 32
TRI_C = 128
WINDOW_AMINOS = 64
WINDOW_HOMOLOGS = 32


def draw_window_amino_flags(key, part):
    length = jax.random.randint(jax.random.fold_in(key, 17), (), WINDOW_AMINOS // 2, WINDOW_AMINOS + 1)
    return (jnp.arange(WINDOW_AMINOS) < length).astype(jnp.int32)


def place_ends(entries, key, low, high):
    longest = entries.shape.index(max(entries.shape))
    spots = []
    for shift in (0, 1):
        where = [jax.random.randint(jax.random.fold_in(key, axis), (), 0, length) for axis, length in enumerate(entries.shape)]
        where[longest] = (where[longest] + shift) % entries.shape[longest]
        spots.append(tuple(where))
    return entries.at[spots[0]].set(low).at[spots[1]].set(high)


def shard_levels(key, dims, cuts, low, top_value):
    def one(axis_at, shards_of):
        steps = jax.random.uniform(jax.random.fold_in(jax.random.fold_in(key, 6), axis_at), (shards_of,), jnp.float32, low / len(cuts), top_value / len(cuts))
        return jnp.repeat(jnp.exp(steps), dims[axis_at] // shards_of).reshape((-1,) + (1,) * (len(dims) - axis_at - 1))

    level = one(*cuts[0])
    for cut in cuts[1:]:
        level = level * one(*cut)
    return level


def gaussian(own_key, dims, deviation, reach, split=(), kind=jnp.bfloat16):
    array = jax.random.normal(own_key, dims, jnp.float32) * deviation
    if len(split) > 0:
        array = shard_levels(own_key, dims, split, -0.22, 0.18) * array
    return jnp.clip(array, min=-reach, max=reach).astype(kind)


def setup_inputs(seed: int = 0, part: int = 0) -> dict:
    keys = jax.random.split(jax.random.key(seed), 18)
    part_splits = jax.random.split(jax.random.fold_in(keys[17], part), 18)
    homolog_matrix = gaussian(part_splits[0], (WINDOW_HOMOLOGS, WINDOW_AMINOS, HOMOLOG_FEATURES), 1.0, 6.0, ((0, 2),))
    homolog_entry_flags = place_ends((jax.random.randint(part_splits[1], (WINDOW_HOMOLOGS, WINDOW_AMINOS), 0, 4) < 3).astype(jnp.int32), jax.random.fold_in(part_splits[1], 1), 0, 1)
    couple_matrix = gaussian(part_splits[2], (WINDOW_AMINOS, WINDOW_AMINOS, CZ), 1.0, 6.0, ((0, 2),))
    window_amino_flags = draw_window_amino_flags(jax.random.fold_in(jax.random.fold_in(keys[17], part), 71), part)
    pairwise_standardize_scaling = jnp.clip(1.0 + 0.18 * jax.random.normal(keys[4], (HOMOLOG_FEATURES,), jnp.float32), 0.1, 1.9)
    pairwise_standardize_offset = gaussian(keys[5], (HOMOLOG_FEATURES,), 0.5, 3.0, (), jnp.float32)
    pairwise_factor_matrices = gaussian(keys[6], (HOMOLOG_FEATURES, 2 * PAIRWISE_FEATURES), HOMOLOG_FEATURES ** -0.5, 0.375)
    pairwise_final_matrix = gaussian(keys[7], (PAIRWISE_FEATURES * PAIRWISE_FEATURES, CZ), (PAIRWISE_FEATURES * PAIRWISE_FEATURES // 16) ** -0.5, 0.75)
    pairwise_final_offset = gaussian(keys[8], (CZ,), 0.5, 3.0, (), jnp.float32)
    trimul_entry_standardize_scaling = jnp.clip(1.0 + 0.18 * jax.random.normal(keys[9], (CZ,), jnp.float32), 0.1, 1.9)
    trimul_entry_standardize_offset = gaussian(keys[10], (CZ,), 0.5, 3.0, (), jnp.float32)
    trimul_entry_matrices = gaussian(keys[11], (CZ, 4 * TRI_C + CZ), CZ ** -0.5, 0.5)
    trimul_entry_offsets = gaussian(keys[12], (4 * TRI_C + CZ,), 0.5, 3.0, (), jnp.float32)
    trimul_final_standardize_scaling = jnp.clip(1.0 + 0.18 * jax.random.normal(keys[13], (TRI_C,), jnp.float32), 0.1, 1.9)
    trimul_final_standardize_offset = gaussian(keys[14], (TRI_C,), 0.5, 3.0, (), jnp.float32)
    trimul_final_matrix = gaussian(keys[15], (TRI_C, CZ), TRI_C ** -0.5, 0.5)
    trimul_final_offset = gaussian(keys[16], (CZ,), 0.5, 3.0, (), jnp.float32)
    return dict(homolog_matrix=homolog_matrix, homolog_entry_flags=homolog_entry_flags, couple_matrix=couple_matrix, window_amino_flags=window_amino_flags, pairwise_standardize_scaling=pairwise_standardize_scaling, pairwise_standardize_offset=pairwise_standardize_offset, pairwise_factor_matrices=pairwise_factor_matrices, pairwise_final_matrix=pairwise_final_matrix, pairwise_final_offset=pairwise_final_offset, trimul_entry_standardize_scaling=trimul_entry_standardize_scaling, trimul_entry_standardize_offset=trimul_entry_standardize_offset, trimul_entry_matrices=trimul_entry_matrices, trimul_entry_offsets=trimul_entry_offsets, trimul_final_standardize_scaling=trimul_final_standardize_scaling, trimul_final_standardize_offset=trimul_final_standardize_offset, trimul_final_matrix=trimul_final_matrix, trimul_final_offset=trimul_final_offset)


def standardize_features(values, gain_vec, bias_vec):
    center = lax.optimization_barrier(jnp.mean(values, axis=-1, keepdims=True))
    rotated_partner_block = values - center
    spread = lax.optimization_barrier(jnp.mean(rotated_partner_block * rotated_partner_block, axis=-1, keepdims=True))
    return rotated_partner_block * lax.rsqrt(spread + 1e-05) * gain_vec + bias_vec

def reference(homolog_matrix, homolog_entry_flags, couple_matrix, window_amino_flags, pairwise_standardize_scaling, pairwise_standardize_offset, pairwise_factor_matrices, pairwise_final_matrix, pairwise_final_offset, trimul_entry_standardize_scaling, trimul_entry_standardize_offset, trimul_entry_matrices, trimul_entry_offsets, trimul_final_standardize_scaling, trimul_final_standardize_offset, trimul_final_matrix, trimul_final_offset):
    residue_present = window_amino_flags.astype(jnp.float32)
    sequence_present = homolog_entry_flags.astype(jnp.float32) * residue_present[None, :]
    homolog_standardized = standardize_features(homolog_matrix.astype(jnp.float32), pairwise_standardize_scaling, pairwise_standardize_offset).astype(jnp.bfloat16)
    mapped_features = jnp.dot(homolog_standardized.reshape(WINDOW_HOMOLOGS * WINDOW_AMINOS, HOMOLOG_FEATURES), pairwise_factor_matrices, preferred_element_type=jnp.float32)
    mapped_features = mapped_features.reshape(WINDOW_HOMOLOGS, WINDOW_AMINOS, 2 * PAIRWISE_FEATURES) * sequence_present[:, :, None]
    outer_product_left_factor = mapped_features[:, :, :PAIRWISE_FEATURES].astype(jnp.bfloat16)
    outer_product_right_factor = mapped_features[:, :, PAIRWISE_FEATURES:].astype(jnp.bfloat16)
    count = jnp.dot(sequence_present.T, sequence_present, precision=lax.Precision.HIGHEST)
    inverse = 1.0 / jnp.maximum(count, 1.0)
    block_rows = 4 if WINDOW_AMINOS % 4 == 0 else 1
    blocks = WINDOW_AMINOS // block_rows
    left_blocks = jnp.transpose(outer_product_left_factor.reshape(WINDOW_HOMOLOGS, blocks, block_rows, PAIRWISE_FEATURES), (1, 0, 2, 3))
    inverse_blocks = inverse.reshape(blocks, block_rows, WINDOW_AMINOS)
    right_wide = outer_product_right_factor.astype(jnp.float32)

    def one_block(inputs):
        left_block, inverse_block = inputs
        products = jnp.einsum('sic,sjd->ijcd', left_block.astype(jnp.float32), right_wide)
        averaged = (products * inverse_block[:, :, None, None]).astype(jnp.bfloat16)
        flat = averaged.reshape(block_rows * WINDOW_AMINOS, PAIRWISE_FEATURES * PAIRWISE_FEATURES)
        update = jnp.dot(flat, pairwise_final_matrix, preferred_element_type=jnp.float32) + pairwise_final_offset
        return update.reshape(block_rows, WINDOW_AMINOS, CZ).astype(jnp.bfloat16)
    opm_update = lax.map(one_block, (left_blocks, inverse_blocks)).reshape(WINDOW_AMINOS, WINDOW_AMINOS, CZ)
    pair_normed = standardize_features(couple_matrix.astype(jnp.float32), trimul_entry_standardize_scaling, trimul_entry_standardize_offset).astype(jnp.bfloat16)
    tri_projected = jnp.dot(pair_normed.reshape(WINDOW_AMINOS * WINDOW_AMINOS, CZ), trimul_entry_matrices, preferred_element_type=jnp.float32) + trimul_entry_offsets
    tri_projected = tri_projected.reshape(WINDOW_AMINOS, WINDOW_AMINOS, 4 * TRI_C + CZ)
    pair_live = (residue_present[:, None] * residue_present[None, :])[:, :, None]
    tri_left = (jax.nn.sigmoid(tri_projected[:, :, :TRI_C]) * tri_projected[:, :, TRI_C:2 * TRI_C] * pair_live).astype(jnp.bfloat16)
    tri_right = (jax.nn.sigmoid(tri_projected[:, :, 2 * TRI_C:3 * TRI_C]) * tri_projected[:, :, 3 * TRI_C:4 * TRI_C] * pair_live).astype(jnp.bfloat16)
    out_gate = jax.nn.sigmoid(tri_projected[:, :, 4 * TRI_C:])
    tri_sum = jnp.einsum('ikc,jkc->ijc', tri_left.astype(jnp.float32), tri_right.astype(jnp.float32))
    tri_mid = standardize_features(tri_sum, trimul_final_standardize_scaling, trimul_final_standardize_offset).astype(jnp.bfloat16)
    mixed = jnp.dot(tri_mid.reshape(WINDOW_AMINOS * WINDOW_AMINOS, TRI_C), trimul_final_matrix, preferred_element_type=jnp.float32).reshape(WINDOW_AMINOS, WINDOW_AMINOS, CZ)
    tri_update = (out_gate * (mixed + trimul_final_offset)).astype(jnp.bfloat16)
    total = couple_matrix.astype(jnp.float32) + opm_update.astype(jnp.float32) + tri_update.astype(jnp.float32)
    return total.astype(jnp.bfloat16)
```

```python
import functools

import jax
import jax.numpy as jnp
from jax import lax
from jax.experimental import pallas as pl
from jax.experimental.pallas import tpu as pltpu
from jax.sharding import PartitionSpec as P

MESH = pl.DeviceIdType.MESH
F32 = jnp.float32
BF16 = jnp.bfloat16
GROUP = 16


def standardize(v, gain, bias):
    center = jnp.mean(v, axis=-1, keepdims=True)
    d = v - center
    spread = jnp.mean(d * d, axis=-1, keepdims=True)
    return d * lax.rsqrt(spread + 1e-05) * gain + bias


def sigmoid(v):
    return 0.5 * jnp.tanh(0.5 * v) + 0.5


def ones_where(shape, test):
    a = lax.broadcasted_iota(jnp.int32, shape, 0)
    b = lax.broadcasted_iota(jnp.int32, shape, 1)
    return jnp.where(test(a, b), 1.0, 0.0).astype(BF16)


def dot(a, b):
    return jnp.dot(a, b, preferred_element_type=F32)


def kernel(
    sizes,
    msa_ref, flags_ref, pair_ref, win_ref, g1_ref, b1_ref, wp_ref, wf_ref, bf_ref,
    g2_ref, b2_ref, wt_ref, bt_ref, g3_ref, b3_ref, wo_ref, bo_ref,
    out_ref,
    xn, ms, xt, osend, orecv, rbuf, rtmp, rk, left, gate, wfs, bd, brow, lo, opm, tri, keep,
    os_sem, or_sem, rs_sem, rr_sem,
):
    D, B, S, N, F, R, C, W, H, E = sizes
    G = C // R
    Q = 128 // W
    T = R // Q
    CH = R // GROUP
    RW, CW = R * W, C * W
    me = lax.axis_index("dap")
    br = lax.axis_index("branch")
    is_owner = lax.div(me, G) == br
    slot = lax.rem(me, G)

    barrier = pltpu.get_barrier_semaphore()
    for o in range(1, D):
        pl.semaphore_signal(
            barrier, inc=1, device_id={"dap": lax.rem(me + o, D)}, device_id_type=MESH
        )
    pl.semaphore_wait(barrier, D - 1)

    col0 = pl.multiple_of(br * C, C)
    win = win_ref[...].astype(F32)
    keep[...] = jnp.broadcast_to(jnp.transpose(jnp.broadcast_to(win, (8, N)))[:, :1], (N, 128))

    def right_copy(o, ch, g):
        rows = pl.ds(pl.multiple_of(g * (R * N) + ch * (GROUP * N), GROUP * N), GROUP * N)
        return pltpu.make_async_remote_copy(
            src_ref=rbuf.at[rows], dst_ref=rbuf.at[rows],
            send_sem=rs_sem.at[o, ch], recv_sem=rr_sem.at[g, ch],
            device_id={"dap": lax.rem(me + o, D)}, device_id_type=MESH,
        )

    def norm_block(blk, carry):
        rows = pl.ds(pl.multiple_of(blk * (4 * N), 4 * N), 4 * N)
        v = pair_ref[rows, :].astype(F32)
        xn[rows, :] = standardize(v, g2_ref[...], b2_ref[...]).astype(BF16)
        return carry

    def row_flags(row):
        return keep[pl.ds(me * R + row, 1), :]

    def right_block(blk, carry):
        rows = pl.ds(pl.multiple_of(blk * (2 * N), 2 * N), 2 * N)
        m = dot(xn[rows, :], wt_ref[:, 2 * H:4 * H]) + bt_ref[:, 2 * H:4 * H]
        v = sigmoid(m[:, :H]) * m[:, H:]
        for u in range(2):
            part = v[u * N:(u + 1) * N] * (keep[...] * row_flags(blk * 2 + u))
            at = pl.multiple_of(slot * (R * N) + (blk * 2 + u) * N, N)
            rbuf[pl.ds(at, N), :] = part.astype(BF16)
        return carry

    for ch in range(CH):
        lax.fori_loop(ch * (GROUP // 4), (ch + 1) * (GROUP // 4), norm_block, 0)

        @pl.when(is_owner)
        def _():
            lax.fori_loop(ch * (GROUP // 2), (ch + 1) * (GROUP // 2), right_block, 0)
            for o in range(1, D):
                right_copy(o, ch, slot).start()

    def msa_block(s, carry):
        rows = pl.ds(pl.multiple_of(s * N, N), N)
        v = msa_ref[rows, :].astype(F32)
        v = standardize(v, g1_ref[...], b1_ref[...])
        for f in range(F // 128):
            ms[f, rows, :] = v[:, f * 128:(f + 1) * 128]
        return carry

    lax.fori_loop(0, S, msa_block, 0)
    for j in range(N):
        for f in range(F // 128):
            xt[j * S:(j + 1) * S, f * 128:(f + 1) * 128] = ms[f, pl.ds(j, S, stride=N), :].astype(BF16)
    live = flags_ref[...].astype(F32) * win
    live_b = live.astype(BF16)
    expand = ones_where((N, N * W), lambda a, b: b // W == a)
    live_wide = dot(live_b, expand)
    place = ones_where((2 * W, 128), lambda a, b: a == b % W)
    place_r = ones_where((2 * W, 128), lambda a, b: a == b % W + W)
    w_left = dot(wp_ref[...], place).astype(BF16)
    w_right = dot(wp_ref[...], place_r).astype(BF16)
    quarter = lax.broadcasted_iota(jnp.int32, (S, 128), 1) // W

    def to_lanes(p, t):
        v = p[t * Q * S:t * Q * S + S]
        for q in range(1, Q):
            v = jnp.where(quarter == q, p[(t * Q + q) * S:(t * Q + q + 1) * S], v)
        return v

    for p in range(D):
        pr = dot(xt[p * R * S:(p + 1) * R * S, :], w_left)
        for t in range(T):
            at = p * RW + t * 128
            osend[p, :, t * 128:(t + 1) * 128] = (
                to_lanes(pr, t) * live_wide[:, at:at + 128]
            ).astype(BF16)
    pr = dot(xt[pl.ds(pl.multiple_of(br * (C * S), C * S), C * S), :], w_right)
    live_cols = dot(live_b, ones_where((N, CW), lambda a, b: b // W + br * C == a))
    right_own = jnp.concatenate(
        [(to_lanes(pr, t) * live_cols[:, t * 128:(t + 1) * 128]).astype(BF16) for t in range(C // Q)],
        axis=1,
    )
    for p in range(D):
        osend[p, :, RW:RW + CW] = right_own
        osend[p, :, RW + CW:RW + CW + N] = live_b

    def opm_copy(o):
        p = lax.rem(me + o, D)
        return pltpu.make_async_remote_copy(
            src_ref=osend.at[p], dst_ref=orecv.at[me],
            send_sem=os_sem.at[o], recv_sem=or_sem.at[o],
            device_id={"dap": p}, device_id_type=MESH,
        )

    for o in range(1, D):
        opm_copy(o).start()
    orecv[me] = osend[me]

    def left_block(blk, carry):
        rows = pl.ds(pl.multiple_of(blk * (2 * N), 2 * N), 2 * N)
        m = dot(xn[rows, :], wt_ref[:, :2 * H]) + bt_ref[:, :2 * H]
        v = sigmoid(m[:, :H]) * m[:, H:]
        for u in range(2):
            part = v[u * N:(u + 1) * N] * (keep[...] * row_flags(blk * 2 + u))
            left[pl.ds(pl.multiple_of((blk * 2 + u) * N, N), N), :] = part.astype(BF16).astype(F32)
            at = pl.multiple_of((blk * 2 + u) * N + col0, C)
            gm = dot(xn[pl.ds(at, C), :], wt_ref[:, 4 * H:]) + bt_ref[:, 4 * H:]
            gate[pl.ds(pl.multiple_of((blk * 2 + u) * C, C), C), :] = sigmoid(gm)
        return carry

    lax.fori_loop(0, R // 2, left_block, 0)

    wfs[...] = wf_ref[...].astype(F32)
    zero = jnp.zeros((W, E), BF16)

    def spread(d, carry):
        w = wfs[pl.ds(d, W, stride=W), :].astype(BF16)
        for q in range(Q):
            at = pl.multiple_of(d * 128 + q * W, W)
            for r in range(Q):
                bd[pl.ds(at, W), r * E:(r + 1) * E] = w if r == q else zero
        return carry

    lax.fori_loop(0, W, spread, 0)

    for o in range(1, D):
        opm_copy(o).wait_recv()
    allv = jnp.concatenate([orecv[p] for p in range(D)], axis=0)
    a_all = allv[:, :RW]
    live_all = allv[:, RW + CW:RW + CW + N]
    brow[...] = jnp.transpose(allv[:, RW:RW + CW].astype(F32))
    for d in range(W):
        o_d = dot(brow[pl.ds(d, C, stride=W), :].astype(BF16), a_all).astype(BF16)
        for t in range(T):
            lo[t * C:(t + 1) * C, d * 128:(d + 1) * 128] = o_d[:, t * 128:(t + 1) * 128]
    cols_t = lax.dot_general(
        ones_where((C, N), lambda a, b: a + br * C == b), live_all,
        (((1,), (1,)), ((), ())), preferred_element_type=F32,
    ).astype(BF16)
    rows_f = dot(live_all, ones_where((N, R), lambda a, b: b + me * R == a)).astype(BF16)
    inverse = 1.0 / jnp.maximum(dot(cols_t, rows_f), 1.0)
    for t in range(T):
        u = dot(lo[t * C:(t + 1) * C, :], bd[...])
        for q in range(Q):
            i = t * Q + q
            v = u[:, q * E:(q + 1) * E] * jnp.broadcast_to(inverse[:, i:i + 1], (C, E)) + bf_ref[...]
            opm[i * C:(i + 1) * C, :] = v.astype(BF16)

    for g in range(G):
        for ch in range(CH):
            source = br * G + g

            @pl.when(source != me)
            def _():
                right_copy(1, ch, g).wait_recv()

            base = g * (R * N) + ch * (GROUP * N)
            for jj in range(GROUP):
                rtmp[jj * N:(jj + 1) * N, :] = rbuf[base + jj * N:base + (jj + 1) * N, :].astype(F32)

            def turn(k, carry):
                rk[pl.ds(pl.multiple_of(k * GROUP, GROUP), GROUP), :] = rtmp[pl.ds(k, GROUP, stride=N), :]
                return carry

            lax.fori_loop(0, N, turn, 0, unroll=8)
            IB = 8

            def tri_block(ib, carry):
                def add(k, accs):
                    v = rk[pl.ds(pl.multiple_of(k * GROUP, GROUP), GROUP), :]
                    return tuple(
                        accs[x] + left[pl.ds((ib * IB + x) * N + k, 1), :] * v for x in range(IB)
                    )

                accs = lax.fori_loop(
                    0, N, add, tuple(jnp.zeros((GROUP, H), F32) for _ in range(IB)), unroll=4
                )
                for x in range(IB):
                    at = pl.multiple_of((ib * IB + x) * C + g * R + ch * GROUP, GROUP)
                    tri[pl.ds(at, GROUP), :] = accs[x]
                return carry

            lax.fori_loop(0, R // IB, tri_block, 0)

    def finish(blk, carry):
        rows = pl.ds(pl.multiple_of(blk * (4 * C), 4 * C), 4 * C)
        mid = standardize(tri[rows, :], g3_ref[...], b3_ref[...]).astype(BF16)
        mixed = dot(mid, wo_ref[...]) + bo_ref[...]
        upd = (gate[rows, :] * mixed).astype(BF16).astype(F32) + opm[rows, :].astype(F32)
        for u in range(4):
            i = blk * 4 + u
            own = pair_ref[pl.ds(pl.multiple_of(i * N + col0, C), C), :].astype(F32)
            out_ref[pl.ds(pl.multiple_of(i * C, C), C), :] = (own + upd[u * C:(u + 1) * C]).astype(BF16)
        return carry

    lax.fori_loop(0, R // 4, finish, 0)

    for o in range(1, D):
        opm_copy(o).wait_send()

        @pl.when(is_owner)
        def _():
            for ch in range(CH):
                right_copy(o, ch, slot).wait_send()


def solution(mesh):
    D, B = mesh.shape["dap"], mesh.shape["branch"]

    def local(msa, flags, pair, win, g1, b1, wp, wf, bf, g2, b2, wt, bt, g3, b3, wo, bo):
        S, N, F = msa.shape
        R, _, E = pair.shape
        H = wo.shape[0]
        W = wp.shape[1] // 2
        C = N // B
        G = C // R
        CH = R // GROUP
        FL = -(-N // 128) * 128
        sizes = (D, B, S, N, F, R, C, W, H, E)
        row = lambda v: v.reshape(1, -1)
        vm = pl.BlockSpec(memory_space=pltpu.VMEM)
        wide = (R + C) * W + FL
        out = pl.pallas_call(
            functools.partial(kernel, sizes),
            out_shape=jax.ShapeDtypeStruct((R * C, E), BF16),
            in_specs=[vm] * 17,
            out_specs=vm,
            scratch_shapes=[
                pltpu.VMEM((R * N, E), BF16),
                pltpu.VMEM((F // 128, S * N, 128), F32),
                pltpu.VMEM((N * S, F), BF16),
                pltpu.VMEM((D, S, wide), BF16),
                pltpu.VMEM((D, S, wide), BF16),
                pltpu.VMEM((C * N, H), BF16),
                pltpu.VMEM((GROUP * N, H), F32),
                pltpu.VMEM((GROUP * N, H), F32),
                pltpu.VMEM((R * N, H), F32),
                pltpu.VMEM((R * C, E), F32),
                pltpu.VMEM((W * W, E), F32),
                pltpu.VMEM((W * 128, (128 // W) * E), BF16),
                pltpu.VMEM((C * W, D * S), F32),
                pltpu.VMEM((R * W // 128 * C, W * 128), BF16),
                pltpu.VMEM((R * C, E), BF16),
                pltpu.VMEM((R * C, H), F32),
                pltpu.VMEM((N, 128), F32),
                pltpu.SemaphoreType.DMA((D,)),
                pltpu.SemaphoreType.DMA((D,)),
                pltpu.SemaphoreType.DMA((D, CH)),
                pltpu.SemaphoreType.DMA((G, CH)),
            ],
            compiler_params=pltpu.CompilerParams(
                collective_id=0, has_side_effects=True, vmem_limit_bytes=56 * 1024 * 1024
            ),
        )(
            msa.reshape(S * N, F), flags, pair.reshape(R * N, E), row(win), row(g1), row(b1), wp, wf,
            row(bf), row(g2), row(b2), wt, row(bt), row(g3), row(b3), wo, row(bo),
        )
        return out.reshape(R, C, E)

    shard = P(("crop", "dap"), None, None)
    placed = (shard, P(("crop", "dap"), None), shard, P("crop")) + (P(),) * 13
    return jax.shard_map(
        local, mesh=mesh, in_specs=placed,
        out_specs=P(("crop", "dap"), "branch", None), check_vma=False,
    )
```

```python
import functools

import jax
import jax.numpy as jnp
from jax import lax
from jax.experimental import pallas as pl
from jax.experimental.pallas import tpu as pltpu
from jax.sharding import PartitionSpec as P

MESH = pl.DeviceIdType.MESH
F32 = jnp.float32
BF16 = jnp.bfloat16
GROUP = 16
PIECE = 8


def standardize(v, gain, bias):
    center = jnp.mean(v, axis=-1, keepdims=True)
    d = v - center
    spread = jnp.mean(d * d, axis=-1, keepdims=True)
    return d * lax.rsqrt(spread + 1e-05) * gain + bias


def sigmoid(v):
    return 0.5 * jnp.tanh(0.5 * v) + 0.5


def ones_where(shape, test):
    a = lax.broadcasted_iota(jnp.int32, shape, 0)
    b = lax.broadcasted_iota(jnp.int32, shape, 1)
    return jnp.where(test(a, b), 1.0, 0.0).astype(BF16)


def dot(a, b):
    return jnp.dot(a, b, preferred_element_type=F32)


def dot_nt(a, b):
    return lax.dot_general(a, b, (((1,), (1,)), ((), ())), preferred_element_type=F32)


def kernel(
    sizes,
    *refs,
):
    hbm, out_ref, vmem, rest = refs[:17], refs[17], refs[18:35], refs[35:]
    (
        msa_ref, flags_ref, pair_ref, win_ref, g1_ref, b1_ref, wp_ref, wf_ref, bf_ref,
        g2_ref, b2_ref, wt_ref, bt_ref, g3_ref, b3_ref, wo_ref, bo_ref,
    ) = vmem
    (
        xn, ms, xt, osend, orecv, rbuf, sbuf, rtmp, rk, left, gate, wfs, bd, brow, bperm, lo, big,
        opm, tri, keep, os_sem, or_sem, rs_sem, rr_sem, in_sem,
    ) = rest
    D, B, S, N, F, R, C, W, H, E = sizes
    G = C // R
    Q = 128 // W
    T = R // Q
    CH = R // PIECE
    per = CH // B
    RW, CW = R * W, C * W
    me = lax.axis_index("dap")
    br = lax.axis_index("branch")
    is_owner = lax.div(me, G) == br
    slot = lax.rem(me, G)

    home = lax.div(me, G)
    share = lax.rem(br - home + B, B)

    barrier = pltpu.get_barrier_semaphore()
    for a in range(B):
        for o in range(D):
            if a or o:
                pl.semaphore_signal(
                    barrier, inc=1,
                    device_id={"dap": lax.rem(me + o, D), "branch": lax.rem(br + a, B)},
                    device_id_type=MESH,
                )

    def load(n):
        return pltpu.make_async_copy(hbm[n], vmem[n], in_sem.at[n])

    first = (2, 9, 10, 11, 12, 3)
    second = (0, 1, 4, 5, 6)
    third = (7, 8, 13, 14, 15, 16)
    for n in first + second + third:
        load(n).start()
    for n in first:
        load(n).wait()

    col0 = pl.multiple_of(br * C, C)
    win = win_ref[...].astype(F32)
    keep[...] = jnp.broadcast_to(jnp.transpose(jnp.broadcast_to(win, (8, N)))[:, :1], (N, 128))

    def right_copy(o, n):
        ch = share * per + n
        return pltpu.make_async_remote_copy(
            src_ref=sbuf.at[n],
            dst_ref=rbuf.at[slot * CH + ch],
            send_sem=rs_sem.at[o, n], recv_sem=rr_sem.at[slot * CH + ch],
            device_id={"dap": lax.rem(me + o, D), "branch": home}, device_id_type=MESH,
        )

    def right_arrival(g, ch):
        return pltpu.make_async_remote_copy(
            src_ref=sbuf.at[0], dst_ref=rbuf.at[g * CH + ch],
            send_sem=rs_sem.at[0, 0], recv_sem=rr_sem.at[g * CH + ch],
            device_id={"dap": lax.rem(me + 1, D)}, device_id_type=MESH,
        )

    def norm_block(blk, carry):
        rows = pl.ds(pl.multiple_of(blk * (4 * N), 4 * N), 4 * N)
        v = pair_ref[rows, :].astype(F32)
        xn[rows, :] = standardize(v, g2_ref[...], b2_ref[...]).astype(BF16)
        return carry

    def row_flags(row):
        return keep[pl.ds(me * R + row, 1), :]

    def right_half(base, u4):
        rows = pl.ds(pl.multiple_of((base + u4 * 4) * N, 4 * N), 4 * N)
        m = dot(xn[rows, :], wt_ref[:, 2 * H:4 * H]) + bias(2 * H, 4 * H)
        v = sigmoid(m[:, :H]) * m[:, H:]
        return [
            (v[u * N:(u + 1) * N] * (keep[...] * row_flags(base + u4 * 4 + u))).astype(BF16)
            for u in range(4)
        ]

    def bias(a, b):
        return bt_ref[:, a:b]

    def norm_piece(ch):
        for u4 in range(PIECE // 4):
            norm_block(ch * (PIECE // 4) + u4, 0)

    def send_piece(n):
        ch = share * per + n
        norm_piece(ch)
        for u4 in range(PIECE // 4):
            for u, part in enumerate(right_half(ch * PIECE, u4)):
                at = (u4 * 4 + u) * N
                sbuf[n, at:at + N, :] = part

        for o in range(1, D):
            right_copy(o, n).start()

        @pl.when(is_owner)
        def _():
            rbuf[slot * CH + ch] = sbuf[n]

    pl.semaphore_wait(barrier, D * B - 1)
    send_piece(0)
    for n in second:
        load(n).wait()

    def msa_block(s, carry):
        rows = pl.ds(pl.multiple_of(s * N, N), N)
        v = msa_ref[rows, :].astype(F32)
        v = standardize(v, g1_ref[...], b1_ref[...])
        for f in range(F // 128):
            ms[f, rows, :] = v[:, f * 128:(f + 1) * 128]
        return carry

    lax.fori_loop(0, S, msa_block, 0)
    for j in range(N):
        for f in range(F // 128):
            xt[j * S:(j + 1) * S, f * 128:(f + 1) * 128] = ms[f, pl.ds(j, S, stride=N), :].astype(BF16)
    live = flags_ref[...].astype(F32) * win
    live_b = live.astype(BF16)
    expand = ones_where((N, N * W), lambda a, b: b // W == a)
    live_wide = dot(live_b, expand)
    place = ones_where((128, 2 * W), lambda a, b: b == a % W)
    place_r = ones_where((128, 2 * W), lambda a, b: b == a % W + W)
    w_left = dot(place, wp_ref[...]).astype(BF16)
    w_right = dot(place_r, wp_ref[...]).astype(BF16)
    quarter = lax.broadcasted_iota(jnp.int32, (S, 128), 1) // W

    def to_lanes(p, t):
        v = p[t * Q * S:t * Q * S + S]
        for q in range(1, Q):
            v = jnp.where(quarter == q, p[(t * Q + q) * S:(t * Q + q + 1) * S], v)
        return v

    for p in range(D):
        pr = dot_nt(xt[p * R * S:(p + 1) * R * S, :], w_left)
        for t in range(T):
            at = p * RW + t * 128
            osend[p, :, t * 128:(t + 1) * 128] = (
                to_lanes(pr, t) * live_wide[:, at:at + 128]
            ).astype(BF16)
    pr = dot_nt(xt[pl.ds(pl.multiple_of(br * (C * S), C * S), C * S), :], w_right)
    live_cols = dot(live_b, ones_where((N, CW), lambda a, b: b // W + br * C == a))
    right_own = jnp.concatenate(
        [(to_lanes(pr, t) * live_cols[:, t * 128:(t + 1) * 128]).astype(BF16) for t in range(C // Q)],
        axis=1,
    )
    for p in range(D):
        osend[p, :, RW:RW + CW] = right_own
        osend[p, :, RW + CW:RW + CW + N] = live_b

    def opm_copy(o):
        p = lax.rem(me + o, D)
        return pltpu.make_async_remote_copy(
            src_ref=osend.at[p], dst_ref=orecv.at[me],
            send_sem=os_sem.at[o], recv_sem=or_sem.at[o],
            device_id={"dap": p}, device_id_type=MESH,
        )

    for o in range(1, D):
        opm_copy(o).start()
    orecv[me] = osend[me]
    for n in range(1, per):
        send_piece(n)

    for a in range(1, B):
        for n in range(per):
            ch = lax.rem(share + a, B) * per + n
            norm_piece(ch)

            @pl.when(is_owner)
            def _():
                for u4 in range(PIECE // 4):
                    for u, part in enumerate(right_half(ch * PIECE, u4)):
                        at = (u4 * 4 + u) * N
                        rbuf[slot * CH + ch, at:at + N, :] = part

    def left_block(blk, carry):
        rows = pl.ds(pl.multiple_of(blk * (4 * N), 4 * N), 4 * N)
        m = dot(xn[rows, :], wt_ref[:, :2 * H]) + bias(0, 2 * H)
        v = sigmoid(m[:, :H]) * m[:, H:]
        for u in range(4):
            part = v[u * N:(u + 1) * N] * (keep[...] * row_flags(blk * 4 + u))
            left[pl.ds(pl.multiple_of((blk * 4 + u) * N, N), N), :] = part.astype(BF16).astype(F32)
        own = jnp.concatenate(
            [xn[pl.ds(pl.multiple_of((blk * 4 + u) * N + col0, C), C), :] for u in range(4)], axis=0
        )
        gm = dot(own, wt_ref[:, 4 * H:]) + bias(4 * H, 4 * H + E)
        gate[pl.ds(pl.multiple_of(blk * 4 * C, 4 * C), 4 * C), :] = sigmoid(gm)
        return carry

    lax.fori_loop(0, R // 4, left_block, 0)
    for n in third:
        load(n).wait()

    wfs[...] = wf_ref[...].astype(F32)
    zero = jnp.zeros((W, E), BF16)

    def spread(d, carry):
        w = wfs[pl.ds(d, W, stride=W), :].astype(BF16)
        for q in range(Q):
            at = pl.multiple_of(d * 128 + q * W, W)
            for r in range(Q):
                bd[pl.ds(at, W), r * E:(r + 1) * E] = w if r == q else zero
        return carry

    lax.fori_loop(0, W, spread, 0, unroll=4)

    for o in range(1, D):
        opm_copy(o).wait_recv()
    allv = jnp.concatenate([orecv[p] for p in range(D)], axis=0)
    a_all = allv[:, :RW]
    live_all = allv[:, RW + CW:RW + CW + N]
    brow[...] = jnp.transpose(allv[:, RW:RW + CW].astype(F32))
    for d in range(W):
        bperm[d * C:(d + 1) * C, :] = brow[pl.ds(d, C, stride=W), :].astype(BF16)
    for t2 in range(T // 2):
        o_t = dot(bperm[...], a_all[:, t2 * 256:(t2 + 1) * 256]).astype(BF16)
        for d in range(W):
            for h in range(2):
                t = t2 * 2 + h
                lo[t * C:(t + 1) * C, d * 128:(d + 1) * 128] = (
                    o_t[d * C:(d + 1) * C, h * 128:(h + 1) * 128]
                )
    cols_t = lax.dot_general(
        ones_where((C, N), lambda a, b: a + br * C == b), live_all,
        (((1,), (1,)), ((), ())), preferred_element_type=F32,
    ).astype(BF16)
    rows_f = dot(live_all, ones_where((N, R), lambda a, b: b + me * R == a)).astype(BF16)
    inverse = 1.0 / jnp.maximum(dot(cols_t, rows_f), 1.0)
    big[...] = dot(lo[...], bd[...])
    for t in range(T):
        u = big[t * C:(t + 1) * C, :]
        for q in range(Q):
            i = t * Q + q
            v = u[:, q * E:(q + 1) * E] * jnp.broadcast_to(inverse[:, i:i + 1], (C, E)) + bf_ref[...]
            opm[i * C:(i + 1) * C, :] = v.astype(BF16)

    for g in range(G):
        for ch in range(R // GROUP):
            source = br * G + g
            pieces = range(ch * (GROUP // PIECE), (ch + 1) * (GROUP // PIECE))

            @pl.when(source != me)
            def _():
                for c2 in pieces:
                    right_arrival(g, c2).wait_recv()

            for x, c2 in enumerate(pieces):
                for jj in range(PIECE):
                    at = (x * PIECE + jj) * N
                    rtmp[at:at + N, :] = rbuf[g * CH + c2, jj * N:(jj + 1) * N, :].astype(F32)

            def turn(k, carry):
                rk[pl.ds(pl.multiple_of(k * GROUP, GROUP), GROUP), :] = rtmp[pl.ds(k, GROUP, stride=N), :]
                return carry

            lax.fori_loop(0, N, turn, 0, unroll=8)
            IB = 8

            def tri_block(ib, carry):
                def add(k, accs):
                    v = rk[pl.ds(pl.multiple_of(k * GROUP, GROUP), GROUP), :]
                    return tuple(
                        accs[x] + left[pl.ds((ib * IB + x) * N + k, 1), :] * v for x in range(IB)
                    )

                accs = lax.fori_loop(
                    0, N, add, tuple(jnp.zeros((GROUP, H), F32) for _ in range(IB)), unroll=4
                )
                for x in range(IB):
                    at = pl.multiple_of((ib * IB + x) * C + g * R + ch * GROUP, GROUP)
                    tri[pl.ds(at, GROUP), :] = accs[x]
                return carry

            lax.fori_loop(0, R // IB, tri_block, 0)

    def finish(blk, carry):
        rows = pl.ds(pl.multiple_of(blk * (4 * C), 4 * C), 4 * C)
        mid = standardize(tri[rows, :], g3_ref[...], b3_ref[...]).astype(BF16)
        mixed = dot(mid, wo_ref[...]) + bo_ref[...]
        upd = (gate[rows, :] * mixed).astype(BF16).astype(F32) + opm[rows, :].astype(F32)
        for u in range(4):
            i = blk * 4 + u
            own = pair_ref[pl.ds(pl.multiple_of(i * N + col0, C), C), :].astype(F32)
            out_ref[pl.ds(pl.multiple_of(i * C, C), C), :] = (own + upd[u * C:(u + 1) * C]).astype(BF16)
        return carry

    lax.fori_loop(0, R // 4, finish, 0)

    for o in range(1, D):
        opm_copy(o).wait_send()
        for n in range(per):
            right_copy(o, n).wait_send()


def solution(mesh):
    D, B = mesh.shape["dap"], mesh.shape["branch"]

    def local(msa, flags, pair, win, g1, b1, wp, wf, bf, g2, b2, wt, bt, g3, b3, wo, bo):
        S, N, F = msa.shape
        R, _, E = pair.shape
        H = wo.shape[0]
        W = wp.shape[1] // 2
        C = N // B
        G = C // R
        CH = R // PIECE
        FL = -(-N // 128) * 128
        sizes = (D, B, S, N, F, R, C, W, H, E)
        row = lambda v: v.reshape(1, -1)
        vm = pl.BlockSpec(memory_space=pltpu.VMEM)
        wide = (R + C) * W + FL
        operands = (
            msa.reshape(S * N, F), flags, pair.reshape(R * N, E), row(win), row(g1), row(b1), wp.T, wf,
            row(bf), row(g2), row(b2), wt, row(bt), row(g3), row(b3), wo, row(bo),
        )
        out = pl.pallas_call(
            functools.partial(kernel, sizes),
            out_shape=jax.ShapeDtypeStruct((R * C, E), BF16),
            in_specs=[pl.BlockSpec(memory_space=pl.ANY)] * 17,
            out_specs=vm,
            scratch_shapes=[pltpu.VMEM(v.shape, v.dtype) for v in operands] + [
                pltpu.VMEM((R * N, E), BF16),
                pltpu.VMEM((F // 128, S * N, 128), F32),
                pltpu.VMEM((N * S, F), BF16),
                pltpu.VMEM((D, S, wide), BF16),
                pltpu.VMEM((D, S, wide), BF16),
                pltpu.VMEM((G * CH, PIECE * N, H), BF16),
                pltpu.VMEM((CH // B, PIECE * N, H), BF16),
                pltpu.VMEM((GROUP * N, H), F32),
                pltpu.VMEM((GROUP * N, H), F32),
                pltpu.VMEM((R * N, H), F32),
                pltpu.VMEM((R * C, E), F32),
                pltpu.VMEM((W * W, E), F32),
                pltpu.VMEM((W * 128, (128 // W) * E), BF16),
                pltpu.VMEM((C * W, D * S), F32),
                pltpu.VMEM((W * C, D * S), BF16),
                pltpu.VMEM((R * W // 128 * C, W * 128), BF16),
                pltpu.VMEM((R * W // 128 * C, (128 // W) * E), F32),
                pltpu.VMEM((R * C, E), BF16),
                pltpu.VMEM((R * C, H), F32),
                pltpu.VMEM((N, 128), F32),
                pltpu.SemaphoreType.DMA((D,)),
                pltpu.SemaphoreType.DMA((D,)),
                pltpu.SemaphoreType.DMA((D, CH // B)),
                pltpu.SemaphoreType.DMA((G * CH,)),
                pltpu.SemaphoreType.DMA((17,)),
            ],
            compiler_params=pltpu.CompilerParams(
                collective_id=0, has_side_effects=True, vmem_limit_bytes=56 * 1024 * 1024
            ),
        )(*operands)
        return out.reshape(R, C, E)

    shard = P(("crop", "dap"), None, None)
    placed = (shard, P(("crop", "dap"), None), shard, P("crop")) + (P(),) * 13
    return jax.shard_map(
        local, mesh=mesh, in_specs=placed,
        out_specs=P(("crop", "dap"), "branch", None), check_vma=False,
    )
```

```python
import functools

import jax
import jax.numpy as jnp
from jax import lax
from jax.experimental import pallas as pl
from jax.experimental.pallas import tpu as pltpu
from jax.sharding import PartitionSpec as P

MESH = pl.DeviceIdType.MESH
F32 = jnp.float32
BF16 = jnp.bfloat16
GROUP = 16
PIECE = 8


def standardize(v, gain, bias):
    center = jnp.mean(v, axis=-1, keepdims=True)
    d = v - center
    spread = jnp.mean(d * d, axis=-1, keepdims=True)
    return d * lax.rsqrt(spread + 1e-05) * gain + bias


def sigmoid(v):
    return 0.5 * jnp.tanh(0.5 * v) + 0.5


def ones_where(shape, test):
    a = lax.broadcasted_iota(jnp.int32, shape, 0)
    b = lax.broadcasted_iota(jnp.int32, shape, 1)
    return jnp.where(test(a, b), 1.0, 0.0).astype(BF16)


def dot(a, b):
    return jnp.dot(a, b, preferred_element_type=F32)


def dot_nt(a, b):
    return lax.dot_general(a, b, (((1,), (1,)), ((), ())), preferred_element_type=F32)


def kernel(
    sizes,
    *refs,
):
    hbm, out_ref, vmem, rest = refs[:17], refs[17], refs[18:35], refs[35:]
    (
        msa_ref, flags_ref, pair_ref, win_ref, g1_ref, b1_ref, wp_ref, wf_ref, bf_ref,
        g2_ref, b2_ref, wt_ref, bt_ref, g3_ref, b3_ref, wo_ref, bo_ref,
    ) = vmem
    (
        xn, ms, xt, osend, orecv, rbuf, sbuf, rtmp, rk, left, gate, wfs, bd, brow, bperm, lo, big,
        opm, tri, keep, os_sem, or_sem, rs_sem, rr_sem, in_sem,
    ) = rest
    D, B, S, N, F, R, C, W, H, E = sizes
    G = C // R
    Q = 128 // W
    T = R // Q
    CH = R // PIECE
    per = CH // B
    RW, CW = R * W, C * W
    me = lax.axis_index("dap")
    br = lax.axis_index("branch")
    is_owner = lax.div(me, G) == br
    slot = lax.rem(me, G)

    home = lax.div(me, G)
    share = lax.rem(br - home + B, B)

    barrier = pltpu.get_barrier_semaphore()
    for a in range(B):
        for o in range(D):
            if a or o:
                pl.semaphore_signal(
                    barrier, inc=1,
                    device_id={"dap": lax.rem(me + o, D), "branch": lax.rem(br + a, B)},
                    device_id_type=MESH,
                )

    def load(n):
        return pltpu.make_async_copy(hbm[n], vmem[n], in_sem.at[n])

    first = (2, 9, 10, 11, 12, 3)
    second = (0, 1, 4, 5, 6)
    third = (7, 8, 13, 14, 15, 16)
    for n in first + second + third:
        load(n).start()

    def clear(d, carry):
        bd[pl.ds(pl.multiple_of(d * 128, 128), 128), :] = jnp.zeros((128, Q * E), BF16)
        return carry

    lax.fori_loop(0, W, clear, 0)
    for n in first:
        load(n).wait()

    col0 = pl.multiple_of(br * C, C)
    win = win_ref[...].astype(F32)
    keep[...] = jnp.broadcast_to(jnp.transpose(jnp.broadcast_to(win, (8, N)))[:, :1], (N, 128))

    def right_copy(o, n):
        ch = share * per + n
        return pltpu.make_async_remote_copy(
            src_ref=sbuf.at[n],
            dst_ref=rbuf.at[slot * CH + ch],
            send_sem=rs_sem.at[o, n], recv_sem=rr_sem.at[slot * CH + ch],
            device_id={"dap": lax.rem(me + o, D), "branch": home}, device_id_type=MESH,
        )

    def right_arrival(g, ch):
        return pltpu.make_async_remote_copy(
            src_ref=sbuf.at[0], dst_ref=rbuf.at[g * CH + ch],
            send_sem=rs_sem.at[0, 0], recv_sem=rr_sem.at[g * CH + ch],
            device_id={"dap": lax.rem(me + 1, D)}, device_id_type=MESH,
        )

    def norm_block(blk, carry):
        rows = pl.ds(pl.multiple_of(blk * (4 * N), 4 * N), 4 * N)
        v = pair_ref[rows, :].astype(F32)
        xn[rows, :] = standardize(v, g2_ref[...], b2_ref[...]).astype(BF16)
        return carry

    def row_flags(row):
        return keep[pl.ds(me * R + row, 1), :]

    def right_half(base, u4):
        rows = pl.ds(pl.multiple_of((base + u4 * 4) * N, 4 * N), 4 * N)
        m = dot(xn[rows, :], wt_ref[:, 2 * H:4 * H]) + bias(2 * H, 4 * H)
        v = sigmoid(m[:, :H]) * m[:, H:]
        return [
            (v[u * N:(u + 1) * N] * (keep[...] * row_flags(base + u4 * 4 + u))).astype(BF16)
            for u in range(4)
        ]

    def bias(a, b):
        return bt_ref[pl.ds(a, b - a)].reshape(1, b - a)

    def norm_piece(ch):
        for u4 in range(PIECE // 4):
            norm_block(ch * (PIECE // 4) + u4, 0)

    def send_piece(n):
        ch = share * per + n
        norm_piece(ch)
        for u4 in range(PIECE // 4):
            for u, part in enumerate(right_half(ch * PIECE, u4)):
                at = (u4 * 4 + u) * N
                sbuf[n, at:at + N, :] = part

        for o in range(1, D):
            right_copy(o, n).start()

        @pl.when(is_owner)
        def _():
            rbuf[slot * CH + ch] = sbuf[n]

    pl.semaphore_wait(barrier, D * B - 1)
    send_piece(0)
    for n in second:
        load(n).wait()

    def msa_block(s, carry):
        rows = pl.ds(pl.multiple_of(s * N, N), N)
        v = msa_ref[rows, :].astype(F32)
        v = standardize(v, g1_ref[...], b1_ref[...])
        for f in range(F // 128):
            ms[f, pl.ds(s * (N + 1), N), :] = v[:, f * 128:(f + 1) * 128]
        return carry

    lax.fori_loop(0, S, msa_block, 0, unroll=2)
    for j in range(N):
        for f in range(F // 128):
            xt[j * S:(j + 1) * S, f * 128:(f + 1) * 128] = ms[f, pl.ds(j, S, stride=N + 1), :].astype(BF16)
    live = flags_ref[...].astype(F32) * win
    live_b = live.astype(BF16)
    expand = ones_where((N, N * W), lambda a, b: b // W == a)
    live_wide = dot(live_b, expand)
    place = ones_where((128, 2 * W), lambda a, b: b == a % W)
    place_r = ones_where((128, 2 * W), lambda a, b: b == a % W + W)
    w_left = dot(place, wp_ref[...]).astype(BF16)
    w_right = dot(place_r, wp_ref[...]).astype(BF16)
    quarter = lax.broadcasted_iota(jnp.int32, (S, 128), 1) // W

    def to_lanes(p, t):
        v = p[t * Q * S:t * Q * S + S]
        for q in range(1, Q):
            v = jnp.where(quarter == q, p[(t * Q + q) * S:(t * Q + q + 1) * S], v)
        return v

    for p in range(D):
        pr = dot_nt(xt[p * R * S:(p + 1) * R * S, :], w_left)
        for t in range(T):
            at = p * RW + t * 128
            osend[p, :, t * 128:(t + 1) * 128] = (
                to_lanes(pr, t) * live_wide[:, at:at + 128]
            ).astype(BF16)
    pr = dot_nt(xt[pl.ds(pl.multiple_of(br * (C * S), C * S), C * S), :], w_right)
    live_cols = dot(live_b, ones_where((N, CW), lambda a, b: b // W + br * C == a))
    right_own = jnp.concatenate(
        [(to_lanes(pr, t) * live_cols[:, t * 128:(t + 1) * 128]).astype(BF16) for t in range(C // Q)],
        axis=1,
    )
    for p in range(D):
        osend[p, :, RW:RW + CW] = right_own
        osend[p, :, RW + CW:RW + CW + N] = live_b

    def opm_copy(o):
        p = lax.rem(me + o, D)
        return pltpu.make_async_remote_copy(
            src_ref=osend.at[p], dst_ref=orecv.at[me],
            send_sem=os_sem.at[o], recv_sem=or_sem.at[o],
            device_id={"dap": p}, device_id_type=MESH,
        )

    for o in range(1, D):
        opm_copy(o).start()
    orecv[me] = osend[me]
    for n in range(1, per):
        send_piece(n)

    for a in range(1, B):
        for n in range(per):
            ch = lax.rem(share + a, B) * per + n
            norm_piece(ch)

            @pl.when(is_owner)
            def _():
                for u4 in range(PIECE // 4):
                    for u, part in enumerate(right_half(ch * PIECE, u4)):
                        at = (u4 * 4 + u) * N
                        rbuf[slot * CH + ch, at:at + N, :] = part

    def left_block(blk, carry):
        rows = pl.ds(pl.multiple_of(blk * (4 * N), 4 * N), 4 * N)
        m = dot(xn[rows, :], wt_ref[:, :2 * H]) + bias(0, 2 * H)
        v = sigmoid(m[:, :H]) * m[:, H:]
        for u in range(4):
            part = v[u * N:(u + 1) * N] * (keep[...] * row_flags(blk * 4 + u))
            left[pl.ds(pl.multiple_of((blk * 4 + u) * N, N), N), :] = part.astype(BF16).astype(F32)
        own = jnp.concatenate(
            [xn[pl.ds(pl.multiple_of((blk * 4 + u) * N + col0, C), C), :] for u in range(4)], axis=0
        )
        gm = dot(own, wt_ref[:, 4 * H:]) + bias(4 * H, 4 * H + E)
        gate[pl.ds(pl.multiple_of(blk * 4 * C, 4 * C), 4 * C), :] = sigmoid(gm)
        return carry

    lax.fori_loop(0, R // 4, left_block, 0)
    for n in third:
        load(n).wait()

    for c in range(W):
        wfs[c * (W + 1):c * (W + 1) + W, :] = wf_ref[c * W:(c + 1) * W, :].astype(F32)

    def spread(d, carry):
        w = wfs[pl.ds(d, W, stride=W + 1), :].astype(BF16)
        for q in range(Q):
            at = pl.multiple_of(d * 128 + q * W, W)
            bd[pl.ds(at, W), q * E:(q + 1) * E] = w
        return carry

    lax.fori_loop(0, W, spread, 0, unroll=4)

    for o in range(1, D):
        opm_copy(o).wait_recv()
    allv = jnp.concatenate([orecv[p] for p in range(D)], axis=0)
    a_all = allv[:, :RW]
    live_all = allv[:, RW + CW:RW + CW + N]
    turned = jnp.transpose(allv[:, RW:RW + CW].astype(F32))
    for j in range(C):
        brow[j * (W + 1):j * (W + 1) + W, :] = turned[j * W:(j + 1) * W]
    for d in range(W):
        bperm[d * C:(d + 1) * C, :] = brow[pl.ds(d, C, stride=W + 1), :].astype(BF16)
    for t2 in range(T // 2):
        o_t = dot(bperm[...], a_all[:, t2 * 256:(t2 + 1) * 256]).astype(BF16)
        for d in range(W):
            for h in range(2):
                t = t2 * 2 + h
                lo[t * C:(t + 1) * C, d * 128:(d + 1) * 128] = (
                    o_t[d * C:(d + 1) * C, h * 128:(h + 1) * 128]
                )
    cols_t = lax.dot_general(
        ones_where((C, N), lambda a, b: a + br * C == b), live_all,
        (((1,), (1,)), ((), ())), preferred_element_type=F32,
    ).astype(BF16)
    rows_f = dot(live_all, ones_where((N, R), lambda a, b: b + me * R == a)).astype(BF16)
    inverse = 1.0 / jnp.maximum(dot(cols_t, rows_f), 1.0)
    big[...] = dot(lo[...], bd[...])
    for t in range(T):
        u = big[t * C:(t + 1) * C, :]
        for q in range(Q):
            i = t * Q + q
            v = u[:, q * E:(q + 1) * E] * jnp.broadcast_to(inverse[:, i:i + 1], (C, E)) + bf_ref[...]
            opm[i * C:(i + 1) * C, :] = v.astype(BF16)

    for g in range(G):
        for ch in range(R // GROUP):
            source = br * G + g
            pieces = range(ch * (GROUP // PIECE), (ch + 1) * (GROUP // PIECE))

            @pl.when(source != me)
            def _():
                for c2 in pieces:
                    right_arrival(g, c2).wait_recv()

            for x, c2 in enumerate(pieces):
                for jj in range(PIECE):
                    at = (x * PIECE + jj) * (N + 1)
                    rtmp[at:at + N, :] = rbuf[g * CH + c2, jj * N:(jj + 1) * N, :].astype(F32)

            def turn(k, carry):
                rk[pl.ds(pl.multiple_of(k * GROUP, GROUP), GROUP), :] = rtmp[pl.ds(k, GROUP, stride=N + 1), :]
                return carry

            lax.fori_loop(0, N, turn, 0, unroll=8)
            IB = 8

            def tri_block(ib, carry):
                def add(k, accs):
                    v = rk[pl.ds(pl.multiple_of(k * GROUP, GROUP), GROUP), :]
                    return tuple(
                        accs[x] + left[pl.ds((ib * IB + x) * N + k, 1), :] * v for x in range(IB)
                    )

                accs = lax.fori_loop(
                    0, N, add, tuple(jnp.zeros((GROUP, H), F32) for _ in range(IB)), unroll=4
                )
                for x in range(IB):
                    at = pl.multiple_of((ib * IB + x) * C + g * R + ch * GROUP, GROUP)
                    tri[pl.ds(at, GROUP), :] = accs[x]
                return carry

            lax.fori_loop(0, R // IB, tri_block, 0)

    def finish(blk, carry):
        rows = pl.ds(pl.multiple_of(blk * (4 * C), 4 * C), 4 * C)
        mid = standardize(tri[rows, :], g3_ref[...], b3_ref[...]).astype(BF16)
        mixed = dot(mid, wo_ref[...]) + bo_ref[...]
        upd = (gate[rows, :] * mixed).astype(BF16).astype(F32) + opm[rows, :].astype(F32)
        for u in range(4):
            i = blk * 4 + u
            own = pair_ref[pl.ds(pl.multiple_of(i * N + col0, C), C), :].astype(F32)
            out_ref[pl.ds(pl.multiple_of(i * C, C), C), :] = (own + upd[u * C:(u + 1) * C]).astype(BF16)
        return carry

    lax.fori_loop(0, R // 4, finish, 0, unroll=2)

    for o in range(1, D):
        opm_copy(o).wait_send()
        for n in range(per):
            right_copy(o, n).wait_send()


def solution(mesh):
    D, B = mesh.shape["dap"], mesh.shape["branch"]

    def local(msa, flags, pair, win, g1, b1, wp, wf, bf, g2, b2, wt, bt, g3, b3, wo, bo):
        S, N, F = msa.shape
        R, _, E = pair.shape
        H = wo.shape[0]
        W = wp.shape[1] // 2
        C = N // B
        G = C // R
        CH = R // PIECE
        FL = -(-N // 128) * 128
        sizes = (D, B, S, N, F, R, C, W, H, E)
        row = lambda v: v.reshape(1, -1)
        vm = pl.BlockSpec(memory_space=pltpu.VMEM)
        wide = (R + C) * W + FL
        operands = (
            msa.reshape(S * N, F), flags, pair.reshape(R * N, E), row(win), row(g1), row(b1), wp.T, wf,
            row(bf), row(g2), row(b2), wt, bt, row(g3), row(b3), wo, row(bo),
        )
        out = pl.pallas_call(
            functools.partial(kernel, sizes),
            out_shape=jax.ShapeDtypeStruct((R * C, E), BF16),
            in_specs=[pl.BlockSpec(memory_space=pl.ANY)] * 17,
            out_specs=vm,
            scratch_shapes=[pltpu.VMEM(v.shape, v.dtype) for v in operands] + [
                pltpu.VMEM((R * N, E), BF16),
                pltpu.VMEM((F // 128, S * (N + 1), 128), F32),
                pltpu.VMEM((N * S, F), BF16),
                pltpu.VMEM((D, S, wide), BF16),
                pltpu.VMEM((D, S, wide), BF16),
                pltpu.VMEM((G * CH, PIECE * N, H), BF16),
                pltpu.VMEM((CH // B, PIECE * N, H), BF16),
                pltpu.VMEM((GROUP * (N + 1), H), F32),
                pltpu.VMEM((GROUP * N, H), F32),
                pltpu.VMEM((R * N, H), F32),
                pltpu.VMEM((R * C, E), F32),
                pltpu.VMEM((W * (W + 1), E), F32),
                pltpu.VMEM((W * 128, (128 // W) * E), BF16),
                pltpu.VMEM((C * (W + 1), D * S), F32),
                pltpu.VMEM((W * C, D * S), BF16),
                pltpu.VMEM((R * W // 128 * C, W * 128), BF16),
                pltpu.VMEM((R * W // 128 * C, (128 // W) * E), F32),
                pltpu.VMEM((R * C, E), BF16),
                pltpu.VMEM((R * C, H), F32),
                pltpu.VMEM((N, 128), F32),
                pltpu.SemaphoreType.DMA((D,)),
                pltpu.SemaphoreType.DMA((D,)),
                pltpu.SemaphoreType.DMA((D, CH // B)),
                pltpu.SemaphoreType.DMA((G * CH,)),
                pltpu.SemaphoreType.DMA((17,)),
            ],
            compiler_params=pltpu.CompilerParams(
                collective_id=0, has_side_effects=True, vmem_limit_bytes=56 * 1024 * 1024
            ),
        )(*operands)
        return out.reshape(R, C, E)

    shard = P(("crop", "dap"), None, None)
    placed = (shard, P(("crop", "dap"), None), shard, P("crop")) + (P(),) * 13
    return jax.shard_map(
        local, mesh=mesh, in_specs=placed,
        out_specs=P(("crop", "dap"), "branch", None), check_vma=False,
    )
```
